256 devices in a mesh: seq: 32 (over x, z_hi, y), rep: 8 (over z_lo, core).
Axes of the slice: x: 4, y: 4, z: 8 (z_hi: 2, z_lo: 4; z = z_hi * 4 + z_lo), core: 2. Of those that a mesh axis runs over, the one named last changes fastest.
Arguments:
- tokens: bfloat16 [16, 96, 180, 768], P('rep', 'seq'), may hold values from -6 to 6
- cotangent: bfloat16 [16, 96, 180, 768], P('rep', 'seq'), may hold values from -6 to 6
- in_weight: bfloat16 [2, 8, 96, 96], replicated, may hold values from -0.21875 to 0.21875
- in_bias: float32 [2, 768], replicated, may hold values from -0.6 to 0.6
- out_weight: bfloat16 [2, 8, 96, 96], replicated, may hold values from -0.21875 to 0.21875
- out_bias: float32 [2, 768], replicated, may hold values from -0.12 to 0.12
Outputs:
- mixed_out: bfloat16 [16, 96, 180, 768], P('rep', 'seq')
- tokens_grad: bfloat16 [16, 96, 180, 768], P('rep', 'seq')
- in_weight_grad: float32 [2, 8, 96, 96], replicated
- in_bias_grad: float32 [2, 768], replicated
- out_weight_grad: float32 [2, 8, 96, 96], replicated
- out_bias_grad: float32 [2, 768], replicated
The draws below stay inside these ranges and needn't reach their ends.
All inputs are finite; a program needn't handle non-finite values.
Results may differ from the reference program's by a relative error of at most 0.0094.
Values may be sent and summed in bfloat16 or wider, within the bound.
A program may use at most 64 MiB of HBM per device.

```python
import math
import jax
import jax.numpy as jnp
from jax import lax

D = 768
BLOCKS = 8
BLOCK = 96
COLS = 180
MODES = 64
ROWS = 96
BATCH = 16


def shard_levels(key, extent, cuts, low, largest):
    def one(axis_at, shards_of):
        heights = jax.random.uniform(jax.random.fold_in(jax.random.fold_in(key, 6), axis_at), (shards_of,), jnp.float32, low / len(cuts), largest / len(cuts))
        return jnp.repeat(jnp.exp(heights), extent[axis_at] // shards_of).reshape((-1,) + (1,) * (len(extent) - axis_at - 1))

    factor_of = one(*cuts[0])
    for cut in cuts[1:]:
        factor_of = factor_of * one(*cut)
    return factor_of


def scatter_about(key, dims, width, limit, pieces=(), kind=jnp.bfloat16):
    drawn = width * jax.random.normal(key, dims, jnp.float32)
    if pieces:
        drawn = drawn * shard_levels(key, dims, pieces, -0.22, 0.18)
    return jnp.clip(drawn, -limit, limit).astype(kind)


def setup_inputs(seed: int = 0) -> dict:
    splits = jax.random.split(jax.random.key(seed), 7)
    tokens = scatter_about(splits[0], (BATCH, ROWS, COLS, D), 1.0, 6.0, ((0, 8), (1, 32)))
    cotangent = scatter_about(splits[1], (BATCH, ROWS, COLS, D), 1.0, 6.0, ((0, 8), (1, 32)))
    in_weight = scatter_about(splits[2], (2, BLOCKS, BLOCK, BLOCK), (8 * BLOCK) ** -0.5, 0.21875)
    in_bias = scatter_about(splits[3], (2, D), 0.1, 0.6, (), jnp.float32)
    out_weight = scatter_about(splits[4], (2, BLOCKS, BLOCK, BLOCK), (8 * BLOCK) ** -0.5, 0.21875)
    out_bias = scatter_about(splits[5], (2, D), 0.02, 0.12, (), jnp.float32)
    return {"tokens": tokens, "cotangent": cotangent, "in_weight": in_weight, "in_bias": in_bias, "out_weight": out_weight, "out_bias": out_bias}


def widen(operand):
    return operand.astype(jnp.float32)

def grid_tables(length, modes):
    position = jnp.arange(length, dtype=jnp.int32)
    frequency = jnp.arange(modes, dtype=jnp.int32)
    residue = position[:, None] * frequency[None, :] % length
    angles = residue.astype(jnp.float32) * (2.0 * math.pi / length)
    factor = 1.0 / math.sqrt(length)
    cosine_table = (jnp.cos(angles) * factor).astype(jnp.bfloat16)
    sine_table = (jnp.sin(angles) * factor).astype(jnp.bfloat16)
    return (cosine_table, sine_table)

def column_tables(grid_width, modes):
    cosine_table, sine_table = grid_tables(grid_width, modes)
    forward = jnp.stack([cosine_table, -sine_table], axis=2)
    doubling = jnp.where(jnp.arange(modes) == 0, 1.0, 2.0).astype(jnp.bfloat16)[:, None]
    inverse = jnp.stack([cosine_table.T * doubling, -(sine_table.T * doubling)], axis=1)
    return (forward, inverse)

def row_table(length):
    cosine_table, sine_table = grid_tables(length, length)
    upper_rows = jnp.stack([cosine_table, sine_table], axis=2)
    lower_rows = jnp.stack([-sine_table, cosine_table], axis=2)
    return jnp.stack([upper_rows, lower_rows], axis=1)

def block_weights(weight):
    real_part, imag_part = (weight[0], weight[1])
    upper_half = jnp.stack([real_part, imag_part], axis=2)
    lower_half = jnp.stack([-imag_part, real_part], axis=2)
    return jnp.stack([upper_half, lower_half], axis=1)

def fold_blocks(blockwise):
    real_part = blockwise[:, 0, :, 0, :] + blockwise[:, 1, :, 1, :]
    imag_part = blockwise[:, 0, :, 1, :] - blockwise[:, 1, :, 0, :]
    return jnp.stack([real_part, imag_part])

def reference(tokens, cotangent, in_weight, in_bias, out_weight, out_bias):
    column_forward, column_inverse = column_tables(COLS, MODES)
    row_matrix = row_table(ROWS)
    weights_in = block_weights(in_weight)
    weights_out = block_weights(out_weight)
    bias_in = in_bias.reshape(2, BLOCKS, BLOCK)
    bias_out = out_bias.reshape(2, BLOCKS, BLOCK)
    mode_count = ROWS * MODES

    def one_sample(pair):
        sample_tokens, sample_cotangent = pair
        spec_rows = jnp.einsum('hwd,wkc->hkcd', widen(sample_tokens), widen(column_forward)).astype(jnp.bfloat16)
        spectrum = jnp.einsum('qehc,hkcd->qked', widen(row_matrix), widen(spec_rows)).astype(jnp.bfloat16)
        flat_modes = spectrum.reshape(mode_count, 2, BLOCKS, BLOCK)
        hidden_pre = jnp.einsum('mcbi,bciej->mebj', widen(flat_modes), widen(weights_in)) + bias_in
        hidden = jax.nn.gelu(hidden_pre).astype(jnp.bfloat16)
        spectrum_out = (jnp.einsum('mcbi,bciej->mebj', widen(hidden), widen(weights_out)) + bias_out).astype(jnp.bfloat16)
        back_rows = jnp.einsum('qehc,qked->hkcd', widen(row_matrix), widen(spectrum_out.reshape(ROWS, MODES, 2, D))).astype(jnp.bfloat16)
        mixed = (widen(sample_tokens) + jnp.einsum('hkcd,kcw->hwd', widen(back_rows), widen(column_inverse))).astype(jnp.bfloat16)
        cot_rows = jnp.einsum('hwd,kcw->hkcd', widen(sample_cotangent), widen(column_inverse)).astype(jnp.bfloat16)
        incoming = jnp.einsum('qehc,hkcd->qked', widen(row_matrix), widen(cot_rows)).astype(jnp.bfloat16)
        incoming = incoming.reshape(mode_count, 2, BLOCKS, BLOCK)
        out_bias_part = lax.optimization_barrier(jnp.sum(widen(incoming), axis=0)).reshape(2, D)
        out_weight_part = fold_blocks(jnp.einsum('mcbi,mebj->bciej', widen(hidden), widen(incoming)))
        hidden_grad = jnp.einsum('mebj,bciej->mcbi', widen(incoming), widen(weights_out))
        pre_grad = jax.vjp(jax.nn.gelu, hidden_pre)[1](hidden_grad)[0].astype(jnp.bfloat16)
        in_bias_part = lax.optimization_barrier(jnp.sum(widen(pre_grad), axis=0)).reshape(2, D)
        in_weight_part = fold_blocks(jnp.einsum('mcbi,mebj->bciej', widen(flat_modes), widen(pre_grad)))
        spectrum_grad = jnp.einsum('mebj,bciej->mcbi', widen(pre_grad), widen(weights_in)).astype(jnp.bfloat16)
        rows_grad = jnp.einsum('qehc,qked->hkcd', widen(row_matrix), widen(spectrum_grad.reshape(ROWS, MODES, 2, D))).astype(jnp.bfloat16)
        grad_tokens = (widen(sample_cotangent) + jnp.einsum('hkcd,wkc->hwd', widen(rows_grad), widen(column_forward))).astype(jnp.bfloat16)
        return (mixed, grad_tokens, in_weight_part, in_bias_part, out_weight_part, out_bias_part)
    outcome = lax.map(one_sample, (tokens, cotangent))
    return (outcome[0], outcome[1], lax.optimization_barrier(jnp.sum(outcome[2], axis=0)) / BATCH, lax.optimization_barrier(jnp.sum(outcome[3], axis=0)) / BATCH, lax.optimization_barrier(jnp.sum(outcome[4], axis=0)) / BATCH, lax.optimization_barrier(jnp.sum(outcome[5], axis=0)) / BATCH)
```

```python
import functools
import math

import jax
import jax.numpy as jnp
import numpy as np
from jax import lax
from jax.experimental import pallas as pl
from jax.experimental.pallas import tpu as pltpu
from jax.sharding import PartitionSpec as P

BF = jnp.bfloat16
F32 = jnp.float32
MESH = pl.DeviceIdType.MESH

SLOTS = 32
PLANE = 16
PIECE = 24
ALL = SLOTS * PIECE
D = 768
HALF = 384
COLS = 180
PADC = 192
ROWS = 96
NT = (((1,), (1,)), ((), ()))
TN = (((0,), (0,)), ((), ()))


def tables(length, modes):
    residue = np.arange(length)[:, None] * np.arange(modes)[None, :] % length
    angles = residue.astype(np.float32) * np.float32(2.0 * math.pi / length)
    factor = np.float32(1.0 / math.sqrt(length))
    return np.cos(angles) * factor, np.sin(angles) * factor


def constants():
    cos_c, sin_c = tables(COLS, 64)
    col = np.zeros((128, PADC), np.float32)
    col[0::2, :COLS] = cos_c.T
    col[1::2, :COLS] = -sin_c.T
    row = np.arange(ALL)
    slot, mode, grid_row, part = row // 24, row // 6 % 2, row // 2 % 3, row % 2
    pick = np.zeros((ALL, 128), np.float32)
    pick[row, slot * 4 + mode * 2 + part] = 1.0
    cos_r, sin_r = tables(ROWS, ROWS)
    device = slot % 16 // 4 * 8 + slot // 16 * 4 + slot % 4
    h = device * 3 + grid_row
    rows_re = np.where(part[None] == 0, cos_r.T[:, h], sin_r.T[:, h])
    rows_im = np.where(part[None] == 0, -sin_r.T[:, h], cos_r.T[:, h])
    rowmix = np.concatenate([rows_re, rows_im])
    return col, pick, rowmix


def floor_div(v, n):
    return jnp.floor((v.astype(F32) + 0.5) * (1.0 / n)).astype(jnp.int32)


def class_mod4(v, n):
    return floor_div(v, n) & 3


def iota(shape, dim):
    return lax.broadcasted_iota(jnp.int32, shape, dim)


def dot(a, b, dims=(((1,), (0,)), ((), ()))):
    return lax.dot_general(a, b, dims, preferred_element_type=F32)


def kernel(
    tok_hbm, cot_hbm, col_ref, colt_ref, pick_ref, pickt_ref, mix_ref, mixt_ref,
    win_ref, wout_ref, bin_ref, bout_ref,
    mixed_ref, tgrad_ref, grads_ref,
    tok, cot, padded, fwd, inv, mrow, mback, wbd,
    send, recv, spec, dgelu, hid, incpair, prepair, work,
    gsrc, gpeer, grs, gplane, gz, gzsum, gpair, gfin, gzag,
    in_sem, send_sem, recv_sem,
):
    me = lax.axis_index("seq")
    rep = lax.axis_index("rep")
    X, Z, Y = me // 8, (me // 4) % 2, me % 4
    xy = X * 4 + Y
    slot = Z * 16 + xy
    zl, core = rep // 2, rep % 2

    def seq_of(z, p):
        return (p // 4) * 8 + z * 4 + p % 4

    def remote(src, dst, k, **where):
        return pltpu.make_async_remote_copy(
            src_ref=src, dst_ref=dst, send_sem=send_sem.at[k], recv_sem=recv_sem.at[k],
            device_id=where, device_id_type=MESH,
        )

    def take(ref, sem):
        pltpu.make_async_copy(ref, ref, sem).wait()

    loads = []
    for s in range(2):
        for h in range(3):
            loads.append(pltpu.make_async_copy(
                tok_hbm.at[s, h], tok.at[s * 3 + h], in_sem.at[0, s * 3 + h]))
    for s in range(2):
        for h in range(3):
            loads.append(pltpu.make_async_copy(
                cot_hbm.at[s, h], cot.at[s * 3 + h], in_sem.at[1, s * 3 + h]))
    for c in loads:
        c.start()
    for sh in range(6):
        padded[sh * PADC + 176:(sh + 1) * PADC, :] = jnp.zeros((16, D), BF)

    barrier = pltpu.get_barrier_semaphore()

    def greet(t, _):
        p = lax.rem(me + t, SLOTS)
        pl.semaphore_signal(barrier, inc=1, device_id={"seq": p}, device_id_type=MESH)
        return 0

    lax.fori_loop(1, SLOTS, greet, 0)
    pl.semaphore_signal(barrier, inc=1, device_id={"rep": zl * 2 + 1 - core}, device_id_type=MESH)
    for t in range(1, 4):
        pl.semaphore_signal(
            barrier, inc=1, device_id={"rep": lax.rem(zl + t, 4) * 2 + core}, device_id_type=MESH)

    picked = dot(pick_ref[...], col_ref[...])
    r = iota((ALL, 1), 0)
    row_sh = class_mod4(r, 12) % 2 * 3 + (floor_div(r, 2) - 3 * floor_div(r, 6))
    for sh in range(6):
        fwd[:, sh * PADC:(sh + 1) * PADC] = jnp.where(row_sh == sh, picked, 0.0).astype(BF)

    pl.semaphore_wait(barrier, SLOTS - 1 + 1 + 3)

    scale_rows = jnp.where((floor_div(r, 24) == 0) & (class_mod4(r, 6) % 2 == 0), 1.0, 2.0)

    def scatter(k):
        def cross(t, _):
            p = lax.rem(xy + t, PLANE)
            remote(send.at[k, (1 - Z) * PLANE + p], recv.at[k, slot], k,
                   seq=seq_of(1 - Z, p)).start()
            return 0

        def near(t, _):
            p = lax.rem(xy + t, PLANE)
            remote(send.at[k, Z * PLANE + p], recv.at[k, slot], k, seq=seq_of(Z, p)).start()
            return 0

        return cross, near

    def store_half(k, z, lhs, rhs, scale):
        left = lhs[pl.ds(pl.multiple_of(z * HALF, HALF), HALF), :]

        def tile(n, _):
            at = pl.ds(pl.multiple_of(n * 256, 256), 256)
            out = dot(left, rhs[:, at])
            if scale is not None:
                out = out * scale
            send[k, pl.ds(z * PLANE, PLANE), :, at] = out.astype(BF).reshape(PLANE, PIECE, 256)
            return 0

        lax.fori_loop(0, 3, tile, 0)

    def exchange(k, lhs, rhs, scale):
        cross, near = scatter(k)
        store_half(k, 1 - Z, lhs, rhs, scale(1 - Z) if scale else None)
        lax.fori_loop(0, PLANE, cross, 0)
        store_half(k, Z, lhs, rhs, scale(Z) if scale else None)
        lax.fori_loop(1, PLANE, near, 0)
        recv[k, slot] = send[k, slot]

    def await_recv(k):
        take(recv.at[k, pl.ds(0, SLOTS - 1)], recv_sem.at[k])

    def await_send(k):
        take(send.at[k, pl.ds(0, SLOTS - 1)], send_sem.at[k])

    def pad(copies, data):
        for sh in range(6):
            copies[sh].wait()
            padded[sh * PADC:sh * PADC + COLS, :] = data[sh]

    pad(loads[:6], tok)
    exchange(0, fwd, padded, None)
    pad(loads[6:], cot)
    rr = iota((HALF, 1), 0)

    def cot_scale(z):
        first = (floor_div(rr, 24) == 0) & (class_mod4(rr, 6) % 2 == 0) & (z == 0)
        return jnp.where(first, 1.0, 2.0)

    exchange(1, fwd, padded, cot_scale)

    c768 = iota((1, ALL), 1)
    col_sh = class_mod4(c768, 12) % 2 * 3 + (floor_div(c768, 2) - 3 * floor_div(c768, 6))
    pickedt = dot(colt_ref[...], pickt_ref[...])
    for sh in range(6):
        inv[sh * PADC:(sh + 1) * PADC, :] = jnp.where(col_sh == sh, pickedt, 0.0).astype(BF)
    col_class = class_mod4(c768, 6)
    row_class = class_mod4(r, 6)
    for e in range(2):
        for cls in range(4):
            at = (e * 4 + cls) * ROWS
            part = mix_ref[e * ROWS:(e + 1) * ROWS, :].astype(F32)
            mrow[at:at + ROWS, :] = jnp.where(col_class == cls, part, 0.0).astype(BF)
    part = mixt_ref[...].astype(F32)
    for e in range(2):
        lane = iota((1, HALF), 1)
        lane_class = floor_div(lane, 96)
        wide = jnp.concatenate([part[:, e * 128:e * 128 + ROWS]] * 4, axis=1)
        mback[:, e * HALF:(e + 1) * HALF] = jnp.where(row_class == lane_class, wide, 0.0).astype(BF)
    lane_block = floor_div(iota((1, HALF), 1), 96)
    for t, ref in enumerate((win_ref, wout_ref)):
        for ri in range(2):
            for g in range(2):
                wide = ref[ri, :, g * HALF:(g + 1) * HALF].astype(F32)
                for n in range(4):
                    wbd[t, ri, g, n * 96:(n + 1) * 96, :] = jnp.where(
                        lane_block == n, wide, 0.0).astype(BF)

    def along_rows(k, store):
        def tile(n, _):
            at = pl.ds(pl.multiple_of(n * 256, 256), 256)
            store(at, dot(mrow[...], recv[k, :, :, at].reshape(ALL, 256)).astype(BF))
            return 0

        lax.fori_loop(0, 3, tile, 0)

    await_recv(0)

    def keep_spec(at, v):
        spec[:, at] = v

    along_rows(0, keep_spec)
    root = math.sqrt(2.0 / math.pi)
    for g in range(2):
        lanes = pl.ds(g * HALF, HALF)
        u = dot(spec[:, lanes], wbd[0, 0, g])
        v = dot(spec[:, lanes], wbd[0, 1, g])
        for e in range(2):
            mine = slice(e * HALF, (e + 1) * HALF)
            if e == 0:
                pre = u[:HALF] - v[HALF:] + bin_ref[0:1, lanes]
            else:
                pre = v[:HALF] + u[HALF:] + bin_ref[1:2, lanes]
            sq = pre * pre
            th = jnp.tanh(root * pre * (1.0 + 0.044715 * sq))
            hid[mine, lanes] = (0.5 * pre * (1.0 + th)).astype(BF)
            dgelu[mine, lanes] = 0.5 * (1.0 + th) + 0.5 * pre * (1.0 - th * th) * (
                root * (1.0 + 3.0 * 0.044715 * sq))
    for g in range(2):
        lanes = pl.ds(g * HALF, HALF)
        u = dot(hid[:, lanes], wbd[1, 0, g])
        v = dot(hid[:, lanes], wbd[1, 1, g])
        work[0:HALF, lanes] = (u[:HALF] - v[HALF:] + bout_ref[0:1, lanes]).astype(BF)
        work[HALF:ALL, lanes] = (v[:HALF] + u[HALF:] + bout_ref[1:2, lanes]).astype(BF)

    def mode_scale(z):
        first = (class_mod4(rr, 6) % 2 == 0) & (slot == 0)
        return jnp.where(first, 1.0, 2.0)

    exchange(2, mback, work, mode_scale)

    await_recv(1)

    def keep_inc(at, v):
        work[:, at] = v

    along_rows(1, keep_inc)

    def pair_up(dst, g, top, bottom):
        dst[g, 0:HALF, 0:HALF] = top
        dst[g, HALF:ALL, 0:HALF] = bottom
        dst[g, 0:HALF, HALF:ALL] = bottom
        dst[g, HALF:ALL, HALF:ALL] = -top

    gsrc[...] = jnp.zeros_like(gsrc)

    def param_grads(t, g, left, pair, bias):
        prod = dot(left[:, g * HALF:(g + 1) * HALF], pair[g], TN)
        for ri in range(2):
            acc = jnp.zeros((96, HALF), F32)
            for n in range(4):
                acc = acc + jnp.where(
                    lane_block == n, prod[n * 96:(n + 1) * 96, ri * HALF:(ri + 1) * HALF], 0.0)
            gsrc[g, t * 8 + ri * 4:t * 8 + ri * 4 + 4, 0:24, :] = acc.reshape(4, 24, HALF)
            gsrc[g, t * 2 + ri, 24:32, :] = jnp.broadcast_to(bias[ri], (8, HALF))

    for g in range(2):
        lanes = pl.ds(g * HALF, HALF)
        inc = work[:, lanes]
        pair_up(incpair, g, inc[:HALF], inc[HALF:])
        u = dot(inc, wbd[1, 0, g], NT)
        v = dot(inc, wbd[1, 1, g], NT)
        top = ((u[:HALF] + v[HALF:]) * dgelu[0:HALF, lanes]).astype(BF)
        bottom = ((u[HALF:] - v[:HALF]) * dgelu[HALF:ALL, lanes]).astype(BF)
        pair_up(prepair, g, top, bottom)
        incf = inc.astype(F32)
        param_grads(1, g, hid, incpair,
                    [jnp.sum(incf[:HALF], axis=0, keepdims=True),
                     jnp.sum(incf[HALF:], axis=0, keepdims=True)])
        param_grads(0, g, spec, prepair,
                    [jnp.sum(top.astype(F32), axis=0, keepdims=True),
                     jnp.sum(bottom.astype(F32), axis=0, keepdims=True)])
    swap = remote(gsrc.at[1 - core], gpeer, 4, rep=zl * 2 + 1 - core)
    swap.start()
    for g in range(2):
        lanes = pl.ds(g * HALF, HALF)
        pre = prepair[g, :, 0:HALF]
        u = dot(pre, wbd[0, 0, g], NT)
        v = dot(pre, wbd[0, 1, g], NT)
        work[0:HALF, lanes] = (u[:HALF] + v[HALF:]).astype(BF)
        work[HALF:ALL, lanes] = (u[HALF:] - v[:HALF]).astype(BF)

    swap.wait_recv()
    grs_own = gsrc.at[core]
    gpeer[...] = gpeer[...] + grs_own[...]

    def reduce_plane(t, _):
        p = lax.rem(xy + t, PLANE)
        remote(gpeer.at[p], grs.at[xy], 5, seq=seq_of(Z, p)).start()
        return 0

    lax.fori_loop(1, PLANE, reduce_plane, 0)
    exchange(3, mback, work, None)

    grs[xy] = gpeer[xy]
    take(grs.at[pl.ds(0, PLANE - 1)], recv_sem.at[5])
    gplane[...] = jnp.sum(grs[...], axis=0).reshape(4, 8, HALF)
    for t in range(1, 4):
        q = lax.rem(zl + t, 4)
        remote(gplane.at[q], gz.at[zl], 6, rep=q * 2 + core).start()
    gz[zl] = gplane[zl]
    take(gz.at[pl.ds(0, 3)], recv_sem.at[6])
    gzsum[...] = jnp.sum(gz[...], axis=0)
    pair = remote(gzsum, gpair, 7, seq=seq_of(1 - Z, xy))
    pair.start()
    pair.wait_recv()
    gfin[...] = (gzsum[...] + gpair[...]) * (1.0 / 16.0)
    for t in range(1, 4):
        q = lax.rem(zl + t, 4)
        remote(gfin, gzag.at[zl], 8, rep=q * 2 + core).start()
    gzag[zl] = gfin[...]
    take(gzag.at[pl.ds(0, 3)], recv_sem.at[8])

    def gather_plane(t, _):
        p = lax.rem(xy + t, PLANE)
        remote(gzag, grads_ref.at[core, xy], 9, seq=seq_of(Z, p)).start()
        return 0

    lax.fori_loop(1, PLANE, gather_plane, 0)
    grads_ref[core, xy] = gzag[...]

    def finish(k, data, out_ref):
        def tile(n, _):
            at = pl.ds(pl.multiple_of(n * 256, 256), 256)
            got = recv[k, :, :, at].reshape(ALL, 256)
            for sh in range(6):
                back = dot(inv[sh * PADC:(sh + 1) * PADC, :], got)
                out_ref[sh // 3, sh % 3, :, at] = (
                    data[sh, :, at].astype(F32) + back[:COLS]).astype(BF)
            return 0

        lax.fori_loop(0, 3, tile, 0)

    await_recv(2)
    finish(2, tok, mixed_ref)

    take(grads_ref.at[core, pl.ds(0, PLANE - 1)], recv_sem.at[9])
    give = remote(grads_ref.at[core], grads_ref.at[core], 10, rep=zl * 2 + 1 - core)
    give.start()

    await_recv(3)
    finish(3, cot, tgrad_ref)
    take(grads_ref.at[1 - core], recv_sem.at[10])

    for k in range(4):
        await_send(k)
    swap.wait_send()
    take(gpeer.at[pl.ds(0, PLANE - 1)], send_sem.at[5])
    take(gplane.at[pl.ds(0, 3)], send_sem.at[6])
    pair.wait_send()
    take(gzag.at[pl.ds(0, 3)], send_sem.at[8])
    take(grads_ref.at[0, pl.ds(0, PLANE - 1)], send_sem.at[9])
    give.wait_send()


def shards(tokens, cotangent, in_weight, in_bias, out_weight, out_bias):
    col, pick, rowmix = constants()
    mixt = np.zeros((ALL, 256), np.float32)
    mixt[:, 0:ROWS] = rowmix[:ROWS].T
    mixt[:, 128:128 + ROWS] = rowmix[ROWS:].T
    const = [jnp.asarray(a, BF) for a in (col, col.T, pick, pick.T, rowmix, mixt)]
    wide = [w.transpose(0, 2, 1, 3).reshape(2, 96, D) for w in (in_weight, out_weight)]
    vm = pl.BlockSpec(memory_space=pltpu.VMEM)
    hb = pl.BlockSpec(memory_space=pl.ANY)
    V = pltpu.VMEM
    grid = tokens.shape
    mixed, tgrad, grads = pl.pallas_call(
        kernel,
        out_shape=(
            jax.ShapeDtypeStruct(grid, BF),
            jax.ShapeDtypeStruct(grid, BF),
            jax.ShapeDtypeStruct((2, PLANE, 4, 8, HALF), F32),
        ),
        in_specs=[hb, hb] + [vm] * 10,
        out_specs=(vm, vm, vm),
        scratch_shapes=[
            V((6, COLS, D), BF), V((6, COLS, D), BF), V((6 * PADC, D), BF),
            V((ALL, 6 * PADC), BF), V((6 * PADC, ALL), BF),
            V((ALL, ALL), BF), V((ALL, ALL), BF),
            V((2, 2, 2, HALF, HALF), BF),
            V((4, SLOTS, PIECE, D), BF), V((4, SLOTS, PIECE, D), BF),
            V((ALL, D), BF), V((ALL, D), F32), V((ALL, D), BF),
            V((2, ALL, ALL), BF), V((2, ALL, ALL), BF), V((ALL, D), BF),
            V((2, PLANE, 32, HALF), F32), V((PLANE, 32, HALF), F32),
            V((PLANE, 32, HALF), F32), V((4, 8, HALF), F32), V((4, 8, HALF), F32),
            V((8, HALF), F32), V((8, HALF), F32), V((8, HALF), F32), V((4, 8, HALF), F32),
            pltpu.SemaphoreType.DMA((2, 6)),
            pltpu.SemaphoreType.DMA((11,)), pltpu.SemaphoreType.DMA((11,)),
        ],
        compiler_params=pltpu.CompilerParams(
            collective_id=0, has_side_effects=True, vmem_limit_bytes=60 * 1024 * 1024),
        name="afno",
    )(tokens, cotangent, *const, *wide, in_bias, out_bias)

    grads = grads.reshape(2, PLANE, 32, HALF)
    full = grads[:, :, 0:24, :].reshape(2, 4, 96, 4, 96).transpose(1, 0, 3, 2, 4)
    full = full.reshape(4, 8, 96, 96)
    bias = grads[:, 0:4, 24, :].transpose(1, 0, 2).reshape(4, D)
    return mixed, tgrad, full[0:2], bias[0:2], full[2:4], bias[2:4]


def solution(mesh):
    in_specs = (P("rep", "seq", None, None), P("rep", "seq", None, None), P(), P(), P(), P())
    out_specs = (P("rep", "seq", None, None), P("rep", "seq", None, None), P(), P(), P(), P())
    return jax.shard_map(shards, mesh=mesh, in_specs=in_specs, out_specs=out_specs, check_vma=False)
```

```python
import functools
import math

import jax
import jax.numpy as jnp
import numpy as np
from jax import lax
from jax.experimental import pallas as pl
from jax.experimental.pallas import tpu as pltpu
from jax.sharding import PartitionSpec as P

BF = jnp.bfloat16
F32 = jnp.float32
MESH = pl.DeviceIdType.MESH

SLOTS = 32
PLANE = 16
PIECE = 24
ALL = SLOTS * PIECE
D = 768
HALF = 384
COLS = 180
PADR = 384
USED = 360
ROWS = 96
FIRST, SECOND = 6, 11
NT = (((1,), (1,)), ((), ()))
TN = (((0,), (0,)), ((), ()))


def tables(length, modes):
    residue = np.arange(length)[:, None] * np.arange(modes)[None, :] % length
    angles = residue.astype(np.float32) * np.float32(2.0 * math.pi / length)
    factor = np.float32(1.0 / math.sqrt(length))
    return np.cos(angles) * factor, np.sin(angles) * factor


def constants():
    cos_c, sin_c = tables(COLS, 64)
    col = np.zeros((128, PADR), np.float32)
    col[0::2, :USED] = np.repeat(cos_c.T, 2, axis=1)
    col[1::2, :USED] = np.repeat(-sin_c.T, 2, axis=1)
    row = np.arange(ALL)
    slot, grid_row, part = row // 24, row // 2 % 3, row % 2
    cos_r, sin_r = tables(ROWS, ROWS)
    device = slot % 16 // 4 * 8 + slot // 16 * 4 + slot % 4
    h = device * 3 + grid_row
    rows_re = np.where(part[None] == 0, cos_r.T[:, h], sin_r.T[:, h])
    rows_im = np.where(part[None] == 0, -sin_r.T[:, h], cos_r.T[:, h])
    mixt = np.zeros((ALL, 256), np.float32)
    mixt[:, 0:ROWS] = rows_re.T
    mixt[:, 128:128 + ROWS] = rows_im.T
    return col, col.T, np.concatenate([rows_re, rows_im]), mixt


def floor_div(v, n):
    return jnp.floor((v.astype(F32) + 0.5) * (1.0 / n)).astype(jnp.int32)


def class_mod4(v, n):
    return floor_div(v, n) & 3


def iota(shape, dim):
    return lax.broadcasted_iota(jnp.int32, shape, dim)


def dot(a, b, dims=(((1,), (0,)), ((), ()))):
    return lax.dot_general(a, b, dims, preferred_element_type=F32)


def kernel(
    tok_hbm, cot_hbm, col_ref, colt_hbm, mix_hbm, mixt_hbm, win_hbm, wout_hbm, bin_ref, bout_ref,
    mixed_hbm, tgrad_hbm, grads_ref,
    tok, cot, tokp, cotp, colt_ref, mix_ref, mixt_ref, wraw, fwd, inv, mrow, mback, wbd,
    send, recv, spec, dgelu, hid, incpair, prepair, work,
    gsrc, gpeer, grs, gplane, gz, gfin, gzag, gout,
    in_sem, table_sem, out_sem, send_sem, recv_sem,
):
    me = lax.axis_index("seq")
    rep = lax.axis_index("rep")
    X, Z, Y = me // 8, (me // 4) % 2, me % 4
    xy = X * 4 + Y
    slot = Z * 16 + xy
    zl, core = rep // 2, rep % 2

    def seq_of(z, p):
        return (p // 4) * 8 + z * 4 + p % 4

    def remote(src, dst, k, **where):
        return pltpu.make_async_remote_copy(
            src_ref=src, dst_ref=dst, send_sem=send_sem.at[k], recv_sem=recv_sem.at[k],
            device_id=where, device_id_type=MESH,
        )

    def take(ref, sem):
        pltpu.make_async_copy(ref, ref, sem).wait()

    loads = [
        [pltpu.make_async_copy(src.at[h], dst.at[h], in_sem.at[i, h]) for h in range(3)]
        for i, (src, dst) in enumerate(((tok_hbm, tok), (cot_hbm, cot)))
    ]
    late = [
        pltpu.make_async_copy(src, dst, table_sem.at[i])
        for i, (src, dst) in enumerate((
            (colt_hbm, colt_ref), (mix_hbm, mix_ref), (mixt_hbm, mixt_ref),
            (win_hbm, wraw.at[0]), (wout_hbm, wraw.at[1])))
    ]
    for c in loads[0] + loads[1] + late:
        c.start()
    for ref in (tokp, cotp):
        for h in range(3):
            ref[h * PADR + 352:(h + 1) * PADR, :] = jnp.zeros((32, D), BF)

    barrier = pltpu.get_barrier_semaphore()

    def greet(t, _):
        p = lax.rem(me + t, SLOTS)
        pl.semaphore_signal(barrier, inc=1, device_id={"seq": p}, device_id_type=MESH)
        return 0

    lax.fori_loop(1, SLOTS, greet, 0)
    pl.semaphore_signal(barrier, inc=1, device_id={"rep": zl * 2 + 1 - core}, device_id_type=MESH)
    z_here = Z * 4 + zl

    def along_z(t):
        z = lax.rem(z_here + t, 8)
        return z, z // 4, z % 4

    def z_peer(t):
        z, hi, lo = along_z(t)
        return {"seq": seq_of(hi, xy), "rep": lo * 2 + core}

    for t in (1, 2, 3, 5, 6, 7):
        pl.semaphore_signal(barrier, inc=1, device_id=z_peer(t), device_id_type=MESH)

    def message_parts(v):
        cls = class_mod4(v, 6)
        pair = floor_div(v, 2)
        grid_row = pair - 3 * floor_div(v, 6)
        table_row = floor_div(v, 24) * 4 + (cls & 1) * 2 + (v & 1)
        return cls, cls >> 1, grid_row, table_row

    r = iota((ALL, 1), 0)
    row_class, row_s, row_h, row_t = message_parts(r)
    pick = jnp.where(iota((ALL, 128), 1) == row_t, 1.0, 0.0).astype(BF)
    picked = dot(pick, col_ref[...])
    picked = jnp.where((iota((1, PADR), 1) & 1) == row_s, picked, 0.0)
    for h in range(3):
        fwd[:, h * PADR:(h + 1) * PADR] = jnp.where(row_h == h, picked, 0.0).astype(BF)

    def pad(copies, data, ref):
        for h in range(3):
            copies[h].wait()
            ref[h * PADR:h * PADR + USED, :] = data[h].reshape(USED, D)

    pad(loads[0], tok, tokp)
    pl.semaphore_wait(barrier, SLOTS - 1 + 1 + 6)

    def cross(k, lo, hi):
        def step(t, _):
            p = lax.rem(xy + t, PLANE)
            remote(send.at[k, (1 - Z) * PLANE + p], recv.at[k, slot], k,
                   seq=seq_of(1 - Z, p)).start()
            return 0

        lax.fori_loop(lo, hi, step, 0)

    def near(k):
        def step(t, _):
            p = lax.rem(xy + t, PLANE)
            remote(send.at[k, Z * PLANE + p], recv.at[k, slot], k, seq=seq_of(Z, p)).start()
            return 0

        lax.fori_loop(1, PLANE, step, 0)

    def store_half(k, z, lhs, rhs, scale):
        left = lhs[pl.ds(pl.multiple_of(z * HALF, HALF), HALF), :]

        def tile(n, _):
            at = pl.ds(pl.multiple_of(n * 256, 256), 256)
            out = dot(left, rhs[:, at])
            if scale is not None:
                out = out * scale
            send[k, pl.ds(z * PLANE, PLANE), :, at] = out.astype(BF).reshape(PLANE, PIECE, 256)
            return 0

        lax.fori_loop(0, 3, tile, 0)

    def exchange(k, lhs, rhs, scale, first=PLANE):
        store_half(k, 1 - Z, lhs, rhs, scale(1 - Z) if scale else None)
        cross(k, 0, first)
        store_half(k, Z, lhs, rhs, scale(Z) if scale else None)
        near(k)
        recv[k, slot] = send[k, slot]

    def await_recv(k):
        take(recv.at[k, pl.ds(0, SLOTS - 1)], recv_sem.at[k])

    def await_send(k):
        take(send.at[k, pl.ds(0, SLOTS - 1)], send_sem.at[k])

    exchange(0, fwd, tokp, None)
    pad(loads[1], cot, cotp)
    rr = iota((HALF, 1), 0)

    def cot_scale(z):
        first = (floor_div(rr, 24) == 0) & (class_mod4(rr, 6) % 2 == 0) & (z == 0)
        return jnp.where(first, 1.0, 2.0)

    exchange(1, fwd, cotp, cot_scale)

    for c in late:
        c.wait()
    c768 = iota((1, ALL), 1)
    col_class, col_s, col_h, col_t = message_parts(c768)
    pickt = jnp.where(iota((128, ALL), 0) == col_t, 1.0, 0.0).astype(BF)
    pickedt = dot(colt_ref[...], pickt)
    pickedt = jnp.where((iota((PADR, 1), 0) & 1) == col_s, pickedt, 0.0)
    for h in range(3):
        inv[h * PADR:(h + 1) * PADR, :] = jnp.where(col_h == h, pickedt, 0.0).astype(BF)
    for e in range(2):
        part = mix_ref[e * ROWS:(e + 1) * ROWS, :].astype(F32)
        for cls in range(4):
            at = (e * 4 + cls) * ROWS
            mrow[at:at + ROWS, :] = jnp.where(col_class == cls, part, 0.0).astype(BF)
    lane_block = floor_div(iota((1, HALF), 1), 96)
    part = mixt_ref[...].astype(F32)
    for e in range(2):
        wide = jnp.concatenate([part[:, e * 128:e * 128 + ROWS]] * 4, axis=1)
        mback[:, e * HALF:(e + 1) * HALF] = jnp.where(row_class == lane_block, wide, 0.0).astype(BF)
    for n in range(4):
        shift = jnp.where(iota((96, HALF), 1) == iota((96, HALF), 0) + 96 * n, 1.0, 0.0).astype(BF)
        for t in range(2):
            for ri in range(2):
                for g in range(2):
                    wbd[t, ri, g, n * 96:(n + 1) * 96, :] = dot(
                        wraw[t, ri, g * 4 + n], shift).astype(BF)

    def along_rows(k, store):
        def tile(n, _):
            at = pl.ds(pl.multiple_of(n * 256, 256), 256)
            store(at, dot(mrow[...], recv[k, :, :, at].reshape(ALL, 256)).astype(BF))
            return 0

        lax.fori_loop(0, 3, tile, 0)

    await_recv(0)

    def keep_spec(at, v):
        spec[:, at] = v

    along_rows(0, keep_spec)
    root = math.sqrt(2.0 / math.pi)
    for g in range(2):
        lanes = pl.ds(g * HALF, HALF)
        u = dot(spec[:, lanes], wbd[0, 0, g])
        v = dot(spec[:, lanes], wbd[0, 1, g])
        for e in range(2):
            mine = slice(e * HALF, (e + 1) * HALF)
            if e == 0:
                pre = u[:HALF] - v[HALF:] + bin_ref[0:1, lanes]
            else:
                pre = v[:HALF] + u[HALF:] + bin_ref[1:2, lanes]
            sq = pre * pre
            th = jnp.tanh(root * pre * (1.0 + 0.044715 * sq))
            hid[mine, lanes] = (0.5 * pre * (1.0 + th)).astype(BF)
            dgelu[mine, lanes] = 0.5 * (1.0 + th) + 0.5 * pre * (1.0 - th * th) * (
                root * (1.0 + 3.0 * 0.044715 * sq))
    for g in range(2):
        lanes = pl.ds(g * HALF, HALF)
        u = dot(hid[:, lanes], wbd[1, 0, g])
        v = dot(hid[:, lanes], wbd[1, 1, g])
        work[0:HALF, lanes] = (u[:HALF] - v[HALF:] + bout_ref[0:1, lanes]).astype(BF)
        work[HALF:ALL, lanes] = (v[:HALF] + u[HALF:] + bout_ref[1:2, lanes]).astype(BF)

    def mode_scale(z):
        first = (class_mod4(rr, 6) % 2 == 0) & (slot == 0)
        return jnp.where(first, 1.0, 2.0)

    exchange(2, mback, work, mode_scale)

    await_recv(1)

    def keep_inc(at, v):
        work[:, at] = v

    along_rows(1, keep_inc)

    def pair_up(dst, g, top, bottom):
        dst[g, 0:HALF, 0:HALF] = top
        dst[g, HALF:ALL, 0:HALF] = bottom
        dst[g, 0:HALF, HALF:ALL] = bottom
        dst[g, HALF:ALL, HALF:ALL] = -top

    gsrc[...] = jnp.zeros_like(gsrc)

    def param_grads(t, g, left, pair, bias):
        prod = dot(left[:, g * HALF:(g + 1) * HALF], pair[g], TN)
        for ri in range(2):
            acc = jnp.zeros((96, HALF), F32)
            for n in range(4):
                acc = acc + jnp.where(
                    lane_block == n, prod[n * 96:(n + 1) * 96, ri * HALF:(ri + 1) * HALF], 0.0)
            gsrc[g, t * 8 + ri * 4:t * 8 + ri * 4 + 4, 0:24, :] = acc.reshape(4, 24, HALF)
            gsrc[g, t * 2 + ri, 24:32, :] = jnp.broadcast_to(bias[ri], (8, HALF))

    for g in range(2):
        lanes = pl.ds(g * HALF, HALF)
        inc = work[:, lanes]
        pair_up(incpair, g, inc[:HALF], inc[HALF:])
        u = dot(inc, wbd[1, 0, g], NT)
        v = dot(inc, wbd[1, 1, g], NT)
        top = ((u[:HALF] + v[HALF:]) * dgelu[0:HALF, lanes]).astype(BF)
        bottom = ((u[HALF:] - v[:HALF]) * dgelu[HALF:ALL, lanes]).astype(BF)
        pair_up(prepair, g, top, bottom)
        incf = inc.astype(F32)
        param_grads(1, g, hid, incpair,
                    [jnp.sum(incf[:HALF], axis=0, keepdims=True),
                     jnp.sum(incf[HALF:], axis=0, keepdims=True)])
        param_grads(0, g, spec, prepair,
                    [jnp.sum(top.astype(F32), axis=0, keepdims=True),
                     jnp.sum(bottom.astype(F32), axis=0, keepdims=True)])
    swap = remote(gsrc.at[1 - core], gpeer, 4, rep=zl * 2 + 1 - core)
    swap.start()
    for g in range(2):
        lanes = pl.ds(g * HALF, HALF)
        pre = prepair[g, :, 0:HALF]
        u = dot(pre, wbd[0, 0, g], NT)
        v = dot(pre, wbd[0, 1, g], NT)
        work[0:HALF, lanes] = (u[:HALF] + v[HALF:]).astype(BF)
        work[HALF:ALL, lanes] = (u[HALF:] - v[:HALF]).astype(BF)

    swap.wait_recv()
    grs_own = gsrc.at[core]
    gpeer[...] = gpeer[...] + grs_own[...]

    def reduce_plane(t, _):
        p = lax.rem(xy + t, PLANE)
        remote(gpeer.at[p], grs.at[xy], 5, seq=seq_of(Z, p)).start()
        return 0

    lax.fori_loop(1, PLANE, reduce_plane, 0)
    exchange(3, mback, work, None, FIRST)

    grs[xy] = gpeer[xy]
    take(grs.at[pl.ds(0, PLANE - 1)], recv_sem.at[5])
    gplane[...] = jnp.sum(grs[...], axis=0).reshape(4, 8, HALF)

    def piece(hi, lo):
        return gplane.at[lo, :, pl.ds(pl.multiple_of(hi * 128, 128), 256)]

    for t in range(1, 8):
        z, hi, lo = along_z(t)
        remote(piece(hi, lo), gz.at[z_here], 6, **z_peer(t)).start()
    cross(3, FIRST, SECOND)
    gz[z_here] = gplane[zl, :, pl.ds(pl.multiple_of(Z * 128, 128), 256)]
    take(gz.at[pl.ds(0, 7)], recv_sem.at[6])
    gfin[...] = jnp.sum(gz[...], axis=0) * (1.0 / 16.0)
    for t in range(1, 8):
        remote(gfin, gzag.at[z_here], 7, **z_peer(t)).start()
    cross(3, SECOND, PLANE)
    gzag[z_here] = gfin[...]
    take(gzag.at[pl.ds(0, 7)], recv_sem.at[7])
    for t in range(4):
        gout[t, :, 0:256] = gzag[t]
        gout[t, :, 256:HALF] = gzag[4 + t, :, 128:256]

    def gather_plane(t, _):
        p = lax.rem(xy + t, PLANE)
        remote(gout, grads_ref.at[core, xy], 8, seq=seq_of(Z, p)).start()
        return 0

    lax.fori_loop(1, PLANE, gather_plane, 0)
    grads_ref[core, xy] = gout[...]

    def finish(k, data, stage, out_hbm):
        copies = []
        for h in range(3):
            def tile(n, _):
                at = pl.ds(pl.multiple_of(n * 256, 256), 256)
                back = dot(inv[h * PADR:(h + 1) * PADR, :], recv[k, :, :, at].reshape(ALL, 256))
                total = data[h * PADR:h * PADR + USED, at].astype(F32) + back[:USED]
                stage[h, :, :, at] = total.astype(BF).reshape(COLS, 2, 256)
                return 0

            lax.fori_loop(0, 3, tile, 0)
            copies.append(pltpu.make_async_copy(stage.at[h], out_hbm.at[h], out_sem.at[k - 2, h]))
            copies[-1].start()
        return copies

    await_recv(2)
    outs = finish(2, tokp, tok, mixed_hbm)

    take(grads_ref.at[core, pl.ds(0, PLANE - 1)], recv_sem.at[8])
    give = remote(grads_ref.at[core], grads_ref.at[core], 9, rep=zl * 2 + 1 - core)
    give.start()

    await_recv(3)
    outs += finish(3, cotp, cot, tgrad_hbm)
    take(grads_ref.at[1 - core], recv_sem.at[9])

    for k in range(4):
        await_send(k)
    swap.wait_send()
    take(gpeer.at[pl.ds(0, PLANE - 1)], send_sem.at[5])
    take(gz.at[pl.ds(0, 7)], send_sem.at[6])
    take(gzag.at[pl.ds(0, 7)], send_sem.at[7])
    take(grads_ref.at[0, pl.ds(0, PLANE - 1)], send_sem.at[8])
    give.wait_send()
    for c in outs:
        c.wait()


def shards(tokens, cotangent, in_weight, in_bias, out_weight, out_bias):
    const = [jnp.asarray(a, BF) for a in constants()]
    vm = pl.BlockSpec(memory_space=pltpu.VMEM)
    hb = pl.BlockSpec(memory_space=pl.ANY)
    V = pltpu.VMEM
    local = (3, COLS, 2, D)
    mixed, tgrad, grads = pl.pallas_call(
        kernel,
        out_shape=(
            jax.ShapeDtypeStruct(local, BF),
            jax.ShapeDtypeStruct(local, BF),
            jax.ShapeDtypeStruct((2, PLANE, 4, 8, HALF), F32),
        ),
        in_specs=[hb, hb, vm, hb, hb, hb, hb, hb, vm, vm],
        out_specs=(hb, hb, vm),
        scratch_shapes=[
            V(local, BF), V(local, BF), V((3 * PADR, D), BF), V((3 * PADR, D), BF),
            V((PADR, 128), BF), V((2 * ROWS, ALL), BF), V((ALL, 256), BF), V((2, 2, 8, 96, 96), BF),
            V((ALL, 3 * PADR), BF), V((3 * PADR, ALL), BF),
            V((ALL, ALL), BF), V((ALL, ALL), BF),
            V((2, 2, 2, HALF, HALF), BF),
            V((4, SLOTS, PIECE, D), BF), V((4, SLOTS, PIECE, D), BF),
            V((ALL, D), BF), V((ALL, D), F32), V((ALL, D), BF),
            V((2, ALL, ALL), BF), V((2, ALL, ALL), BF), V((ALL, D), BF),
            V((2, PLANE, 32, HALF), F32), V((PLANE, 32, HALF), F32),
            V((PLANE, 32, HALF), F32), V((4, 8, HALF), F32), V((8, 8, 256), F32),
            V((8, 256), F32), V((8, 8, 256), F32), V((4, 8, HALF), F32),
            pltpu.SemaphoreType.DMA((2, 3)), pltpu.SemaphoreType.DMA((5,)),
            pltpu.SemaphoreType.DMA((2, 3)),
            pltpu.SemaphoreType.DMA((10,)), pltpu.SemaphoreType.DMA((10,)),
        ],
        compiler_params=pltpu.CompilerParams(
            collective_id=0, has_side_effects=True, vmem_limit_bytes=60 * 1024 * 1024),
        name="afno",
    )(tokens.transpose(1, 2, 0, 3), cotangent.transpose(1, 2, 0, 3), *const,
      in_weight, out_weight, in_bias, out_bias)
    mixed, tgrad = (a.transpose(2, 0, 1, 3) for a in (mixed, tgrad))

    grads = grads.reshape(2, PLANE, 32, HALF)
    full = grads[:, :, 0:24, :].reshape(2, 4, 96, 4, 96).transpose(1, 0, 3, 2, 4)
    full = full.reshape(4, 8, 96, 96)
    bias = grads[:, 0:4, 24, :].transpose(1, 0, 2).reshape(4, D)
    return mixed, tgrad, full[0:2], bias[0:2], full[2:4], bias[2:4]


def solution(mesh):
    in_specs = (P("rep", "seq", None, None), P("rep", "seq", None, None), P(), P(), P(), P())
    out_specs = (P("rep", "seq", None, None), P("rep", "seq", None, None), P(), P(), P(), P())
    return jax.shard_map(shards, mesh=mesh, in_specs=in_specs, out_specs=out_specs, check_vma=False)
```

```python
import functools
import math

import jax
import jax.numpy as jnp
import numpy as np
from jax import lax
from jax.experimental import pallas as pl
from jax.experimental.pallas import tpu as pltpu
from jax.sharding import PartitionSpec as P

BF = jnp.bfloat16
F32 = jnp.float32
MESH = pl.DeviceIdType.MESH

SLOTS = 32
PLANE = 16
PIECE = 24
ALL = SLOTS * PIECE
D = 768
HALF = 384
COLS = 180
PADR = 384
USED = 360
ROWS = 96
WINDOW = 6
NT = (((1,), (1,)), ((), ()))
TN = (((0,), (0,)), ((), ()))


def tables(length, modes):
    residue = np.arange(length)[:, None] * np.arange(modes)[None, :] % length
    angles = residue.astype(np.float32) * np.float32(2.0 * math.pi / length)
    factor = np.float32(1.0 / math.sqrt(length))
    return np.cos(angles) * factor, np.sin(angles) * factor


def constants():
    cos_c, sin_c = tables(COLS, 64)
    col = np.zeros((128, PADR), np.float32)
    col[0::2, :USED] = np.repeat(cos_c.T, 2, axis=1)
    col[1::2, :USED] = np.repeat(-sin_c.T, 2, axis=1)
    row = np.arange(ALL)
    slot, grid_row, part = row // 24, row // 2 % 3, row % 2
    cos_r, sin_r = tables(ROWS, ROWS)
    device = slot % 16 // 4 * 8 + slot // 16 * 4 + slot % 4
    h = device * 3 + grid_row
    rows_re = np.where(part[None] == 0, cos_r.T[:, h], sin_r.T[:, h])
    rows_im = np.where(part[None] == 0, -sin_r.T[:, h], cos_r.T[:, h])
    mixt = np.zeros((ALL, 256), np.float32)
    mixt[:, 0:ROWS] = rows_re.T
    mixt[:, 128:128 + ROWS] = rows_im.T
    return col, col.T, np.concatenate([rows_re, rows_im]), mixt


def floor_div(v, n):
    return jnp.floor((v.astype(F32) + 0.5) * (1.0 / n)).astype(jnp.int32)


def class_mod4(v, n):
    return floor_div(v, n) & 3


def iota(shape, dim):
    return lax.broadcasted_iota(jnp.int32, shape, dim)


def dot(a, b, dims=(((1,), (0,)), ((), ()))):
    return lax.dot_general(a, b, dims, preferred_element_type=F32)


def kernel(
    tok_hbm, cot_hbm, col_ref, colt_hbm, mix_hbm, mixt_hbm, win_hbm, wout_hbm, bin_ref, bout_ref,
    mixed_ref, tgrad_ref, gwin_ref, gbin_ref, gwout_ref, gbout_ref,
    tok, cot, tokp, cotp, grads_ref, colt_ref, mix_ref, mixt_ref, wraw, fwd, inv, mrow, mback, wbd,
    send, recv, spec, dgelu, hid, incpair, prepair, work,
    gsrc, gpeer, grs, gplane, gz, gfin, gzag, gout,
    in_sem, table_sem, cross_sem, send_sem, recv_sem,
):
    me = lax.axis_index("seq")
    rep = lax.axis_index("rep")
    X, Z, Y = me // 8, (me // 4) % 2, me % 4
    xy = X * 4 + Y
    slot = Z * 16 + xy
    zl, core = rep // 2, rep % 2

    def seq_of(z, p):
        return (p // 4) * 8 + z * 4 + p % 4

    def remote(src, dst, k, **where):
        return pltpu.make_async_remote_copy(
            src_ref=src, dst_ref=dst, send_sem=send_sem.at[k], recv_sem=recv_sem.at[k],
            device_id=where, device_id_type=MESH,
        )

    def take(ref, sem):
        pltpu.make_async_copy(ref, ref, sem).wait()

    loads = [
        [pltpu.make_async_copy(src.at[h], dst.at[h], in_sem.at[i, h]) for h in range(3)]
        for i, (src, dst) in enumerate(((tok_hbm, tok), (cot_hbm, cot)))
    ]
    late = [
        pltpu.make_async_copy(src, dst, table_sem.at[i])
        for i, (src, dst) in enumerate((
            (colt_hbm, colt_ref), (mix_hbm, mix_ref), (mixt_hbm, mixt_ref),
            (win_hbm, wraw.at[0]), (wout_hbm, wraw.at[1])))
    ]
    for c in loads[0] + loads[1] + late:
        c.start()
    for ref in (tokp, cotp):
        for h in range(3):
            ref[h * PADR + 352:(h + 1) * PADR, :] = jnp.zeros((32, D), BF)

    barrier = pltpu.get_barrier_semaphore()

    def greet(t, _):
        p = lax.rem(me + t, SLOTS)
        pl.semaphore_signal(barrier, inc=1, device_id={"seq": p}, device_id_type=MESH)
        return 0

    lax.fori_loop(1, SLOTS, greet, 0)
    pl.semaphore_signal(barrier, inc=1, device_id={"rep": zl * 2 + 1 - core}, device_id_type=MESH)
    z_here = Z * 4 + zl

    def along_z(t):
        z = lax.rem(z_here + t, 8)
        return z, z // 4, z % 4

    def z_peer(t):
        z, hi, lo = along_z(t)
        return {"seq": seq_of(hi, xy), "rep": lo * 2 + core}

    for t in (1, 2, 3, 5, 6, 7):
        pl.semaphore_signal(barrier, inc=1, device_id=z_peer(t), device_id_type=MESH)

    def message_parts(v):
        cls = class_mod4(v, 6)
        pair = floor_div(v, 2)
        grid_row = pair - 3 * floor_div(v, 6)
        table_row = floor_div(v, 24) * 4 + (cls & 1) * 2 + (v & 1)
        return cls, cls >> 1, grid_row, table_row

    r = iota((ALL, 1), 0)
    row_class, row_s, row_h, row_t = message_parts(r)
    pick = jnp.where(iota((ALL, 128), 1) == row_t, 1.0, 0.0).astype(BF)
    picked = dot(pick, col_ref[...])
    picked = jnp.where((iota((1, PADR), 1) & 1) == row_s, picked, 0.0)
    for h in range(3):
        fwd[:, h * PADR:(h + 1) * PADR] = jnp.where(row_h == h, picked, 0.0).astype(BF)

    def pad(copies, data, ref):
        for h in range(3):
            copies[h].wait()
            ref[h * PADR:h * PADR + USED, :] = data[h].reshape(USED, D)

    pad(loads[0], tok, tokp)
    pl.semaphore_wait(barrier, SLOTS - 1 + 1 + 6)

    def await_cross(k, t):
        pltpu.make_async_copy(send.at[k, 0], send.at[k, 0], cross_sem.at[k, t]).wait()

    def cross(k, lo, hi, paced=False):
        def step(t, _):
            if paced:
                before = k * PLANE + t - WINDOW
                await_cross(before // PLANE, before % PLANE)
            p = lax.rem(xy + t, PLANE)
            pltpu.make_async_remote_copy(
                src_ref=send.at[k, (1 - Z) * PLANE + p], dst_ref=recv.at[k, slot],
                send_sem=cross_sem.at[k, t], recv_sem=recv_sem.at[k],
                device_id={"seq": seq_of(1 - Z, p)}, device_id_type=MESH).start()
            return 0

        lax.fori_loop(lo, hi, step, 0)

    def near(k):
        def step(t, _):
            p = lax.rem(xy + t, PLANE)
            remote(send.at[k, Z * PLANE + p], recv.at[k, slot], k, seq=seq_of(Z, p)).start()
            return 0

        lax.fori_loop(1, PLANE, step, 0)

    def store_half(k, z, lhs, rhs, scale):
        left = lhs[pl.ds(pl.multiple_of(z * HALF, HALF), HALF), :]

        def tile(n, _):
            at = pl.ds(pl.multiple_of(n * 256, 256), 256)
            out = dot(left, rhs[:, at])
            if scale is not None:
                out = out * scale
            send[k, pl.ds(z * PLANE, PLANE), :, at] = out.astype(BF).reshape(PLANE, PIECE, 256)
            return 0

        lax.fori_loop(0, 3, tile, 0)

    def exchange(k, lhs, rhs, scale, first=PLANE, paced=False, both=True):
        store_half(k, 1 - Z, lhs, rhs, scale(1 - Z) if scale else None)
        cross(k, 0, first, paced)
        store_half(k, Z, lhs, rhs, scale(Z) if scale else None)
        if both:
            near(k)
        recv[k, slot] = send[k, slot]

    def await_recv(k):
        take(recv.at[k, pl.ds(0, SLOTS - 1)], recv_sem.at[k])

    def await_send(k):
        take(send.at[k, pl.ds(0, PLANE - 1)], send_sem.at[k])

    exchange(0, fwd, tokp, None)
    pad(loads[1], cot, cotp)
    rr = iota((HALF, 1), 0)

    def cot_scale(z):
        first = (floor_div(rr, 24) == 0) & (class_mod4(rr, 6) % 2 == 0) & (z == 0)
        return jnp.where(first, 1.0, 2.0)

    held = jnp.where(z_here % 4 == 0, 11, jnp.where(z_here % 4 == 3, 14, PLANE))
    exchange(1, fwd, cotp, cot_scale, held)

    for c in late:
        c.wait()
    c768 = iota((1, ALL), 1)
    col_class, col_s, col_h, col_t = message_parts(c768)
    pickt = jnp.where(iota((128, ALL), 0) == col_t, 1.0, 0.0).astype(BF)
    pickedt = dot(colt_ref[...], pickt)
    pickedt = jnp.where((iota((PADR, 1), 0) & 1) == col_s, pickedt, 0.0)
    for h in range(3):
        inv[h * PADR:(h + 1) * PADR, :] = jnp.where(col_h == h, pickedt, 0.0).astype(BF)
    for e in range(2):
        part = mix_ref[e * ROWS:(e + 1) * ROWS, :].astype(F32)
        for cls in range(4):
            at = (e * 4 + cls) * ROWS
            mrow[at:at + ROWS, :] = jnp.where(col_class == cls, part, 0.0).astype(BF)
    lane_block = floor_div(iota((1, HALF), 1), 96)
    part = mixt_ref[...].astype(F32)
    for e in range(2):
        wide = jnp.concatenate([part[:, e * 128:e * 128 + ROWS]] * 4, axis=1)
        mback[:, e * HALF:(e + 1) * HALF] = jnp.where(row_class == lane_block, wide, 0.0).astype(BF)
    for n in range(4):
        shift = jnp.where(iota((96, HALF), 1) == iota((96, HALF), 0) + 96 * n, 1.0, 0.0).astype(BF)
        for t in range(2):
            for ri in range(2):
                for g in range(2):
                    wbd[t, ri, g, n * 96:(n + 1) * 96, :] = dot(
                        wraw[t, ri, g * 4 + n], shift).astype(BF)

    def along_rows(k, store):
        def tile(n, _):
            at = pl.ds(pl.multiple_of(n * 256, 256), 256)
            store(at, dot(mrow[...], recv[k, :, :, at].reshape(ALL, 256)).astype(BF))
            return 0

        lax.fori_loop(0, 3, tile, 0)

    await_recv(0)

    def keep_spec(at, v):
        spec[:, at] = v

    along_rows(0, keep_spec)
    root = math.sqrt(2.0 / math.pi)
    for g in range(2):
        lanes = pl.ds(g * HALF, HALF)
        u = dot(spec[:, lanes], wbd[0, 0, g])
        v = dot(spec[:, lanes], wbd[0, 1, g])
        for e in range(2):
            mine = slice(e * HALF, (e + 1) * HALF)
            if e == 0:
                pre = u[:HALF] - v[HALF:] + bin_ref[0:1, lanes]
            else:
                pre = v[:HALF] + u[HALF:] + bin_ref[1:2, lanes]
            sq = pre * pre
            th = jnp.tanh(root * pre * (1.0 + 0.044715 * sq))
            hid[mine, lanes] = (0.5 * pre * (1.0 + th)).astype(BF)
            dgelu[mine, lanes] = 0.5 * (1.0 + th) + 0.5 * pre * (1.0 - th * th) * (
                root * (1.0 + 3.0 * 0.044715 * sq))
    for g in range(2):
        lanes = pl.ds(g * HALF, HALF)
        u = dot(hid[:, lanes], wbd[1, 0, g])
        v = dot(hid[:, lanes], wbd[1, 1, g])
        work[0:HALF, lanes] = (u[:HALF] - v[HALF:] + bout_ref[0:1, lanes]).astype(BF)
        work[HALF:ALL, lanes] = (v[:HALF] + u[HALF:] + bout_ref[1:2, lanes]).astype(BF)

    def mode_scale(z):
        first = (class_mod4(rr, 6) % 2 == 0) & (slot == 0)
        return jnp.where(first, 1.0, 2.0)

    exchange(2, mback, work, mode_scale, 0)

    cross(1, held, PLANE)

    await_recv(1)

    def keep_inc(at, v):
        work[:, at] = v

    cross(2, 0, WINDOW)
    along_rows(1, keep_inc)
    cross(2, WINDOW, 8, True)

    def pair_up(dst, g, top, bottom):
        dst[g, 0:HALF, 0:HALF] = top
        dst[g, HALF:ALL, 0:HALF] = bottom
        dst[g, 0:HALF, HALF:ALL] = bottom
        dst[g, HALF:ALL, HALF:ALL] = -top

    gsrc[...] = jnp.zeros_like(gsrc)

    def param_grads(t, g, left, pair, bias):
        prod = dot(left[:, g * HALF:(g + 1) * HALF], pair[g], TN)
        for ri in range(2):
            acc = jnp.zeros((96, HALF), F32)
            for n in range(4):
                acc = acc + jnp.where(
                    lane_block == n, prod[n * 96:(n + 1) * 96, ri * HALF:(ri + 1) * HALF], 0.0)
            gsrc[g, t * 8 + ri * 4:t * 8 + ri * 4 + 4, 0:24, :] = acc.reshape(4, 24, HALF)
            gsrc[g, t * 2 + ri, 24:32, :] = jnp.broadcast_to(bias[ri], (8, HALF))

    for g in range(2):
        lanes = pl.ds(g * HALF, HALF)
        inc = work[:, lanes]
        pair_up(incpair, g, inc[:HALF], inc[HALF:])
        u = dot(inc, wbd[1, 0, g], NT)
        v = dot(inc, wbd[1, 1, g], NT)
        top = ((u[:HALF] + v[HALF:]) * dgelu[0:HALF, lanes]).astype(BF)
        bottom = ((u[HALF:] - v[:HALF]) * dgelu[HALF:ALL, lanes]).astype(BF)
        pair_up(prepair, g, top, bottom)
        cross(2, 8 + 3 * g, 11 + 3 * g, True)
        incf = inc.astype(F32)
        param_grads(1, g, hid, incpair,
                    [jnp.sum(incf[:HALF], axis=0, keepdims=True),
                     jnp.sum(incf[HALF:], axis=0, keepdims=True)])
        param_grads(0, g, spec, prepair,
                    [jnp.sum(top.astype(F32), axis=0, keepdims=True),
                     jnp.sum(bottom.astype(F32), axis=0, keepdims=True)])
    swap = remote(gsrc.at[1 - core], gpeer, 4, rep=zl * 2 + 1 - core)
    swap.start()
    cross(2, 14, PLANE, True)
    for g in range(2):
        lanes = pl.ds(g * HALF, HALF)
        pre = prepair[g, :, 0:HALF]
        u = dot(pre, wbd[0, 0, g], NT)
        v = dot(pre, wbd[0, 1, g], NT)
        work[0:HALF, lanes] = (u[:HALF] + v[HALF:]).astype(BF)
        work[HALF:ALL, lanes] = (u[HALF:] - v[:HALF]).astype(BF)

    swap.wait_recv()
    grs_own = gsrc.at[core]
    gpeer[...] = gpeer[...] + grs_own[...]

    def reduce_plane(t, _):
        p = lax.rem(xy + t, PLANE)
        remote(gpeer.at[p], grs.at[xy], 5, seq=seq_of(Z, p)).start()
        return 0

    lax.fori_loop(1, PLANE, reduce_plane, 0)
    exchange(3, mback, work, None, WINDOW, True, False)

    grs[xy] = gpeer[xy]
    take(grs.at[pl.ds(0, PLANE - 1)], recv_sem.at[5])
    gplane[...] = jnp.sum(grs[...], axis=0).reshape(4, 8, HALF)

    def piece(hi, lo):
        return gplane.at[lo, :, pl.ds(pl.multiple_of(hi * 128, 128), 256)]

    for t in range(1, 8):
        z, hi, lo = along_z(t)
        remote(piece(hi, lo), gz.at[z_here], 6, **z_peer(t)).start()
    near(3)
    cross(3, WINDOW, 10, True)
    gz[z_here] = gplane[zl, :, pl.ds(pl.multiple_of(Z * 128, 128), 256)]
    take(gz.at[pl.ds(0, 7)], recv_sem.at[6])
    gfin[...] = jnp.sum(gz[...], axis=0) * (1.0 / 16.0)
    for t in range(1, 8):
        remote(gfin, gzag.at[z_here], 7, **z_peer(t)).start()
    cross(3, 10, PLANE, True)
    gzag[z_here] = gfin[...]
    take(gzag.at[pl.ds(0, 7)], recv_sem.at[7])
    for t in range(4):
        gout[t, :, 0:256] = gzag[t].astype(BF)
        gout[t, :, 256:HALF] = gzag[4 + t, :, 128:256].astype(BF)

    def gather_plane(t, _):
        p = lax.rem(xy + t, PLANE)
        remote(gout, grads_ref.at[core, xy], 8, seq=seq_of(Z, p)).start()
        return 0

    lax.fori_loop(1, PLANE, gather_plane, 0)
    grads_ref[core, xy] = gout[...]

    def finish(k, data, out_ref):
        def tile(n, _):
            at = pl.ds(pl.multiple_of(n * 256, 256), 256)
            got = recv[k, :, :, at].reshape(ALL, 256)
            for h in range(3):
                back = dot(inv[h * PADR:(h + 1) * PADR, :], got)
                total = data[h * PADR:h * PADR + USED, at].astype(F32) + back[:USED]
                out_ref[h, :, :, at] = total.astype(BF).reshape(COLS, 2, 256)
            return 0

        lax.fori_loop(0, 3, tile, 0)

    def place_grads(g):
        for q in range(4):
            weight, bias = ((gwin_ref, gbin_ref), (gwout_ref, gbout_ref))[q // 2]
            wide = grads_ref[g, 4 * q:4 * q + 4, 0:3].astype(F32).reshape(96, HALF)
            for n in range(4):
                weight[q % 2, g * 4 + n] = wide[:, n * 96:(n + 1) * 96]
            bias[q % 2:q % 2 + 1, pl.ds(pl.multiple_of(g * HALF, 128), HALF)] = (
                grads_ref[g, q, 3].astype(F32)[0:1])

    await_recv(2)
    finish(2, tokp, mixed_ref)

    take(grads_ref.at[core, pl.ds(0, PLANE - 1)], recv_sem.at[8])
    give = remote(grads_ref.at[core], grads_ref.at[core], 9, rep=zl * 2 + 1 - core)
    give.start()
    place_grads(core)
    await_recv(3)
    finish(3, cotp, tgrad_ref)
    take(grads_ref.at[1 - core], recv_sem.at[9])
    place_grads(1 - core)

    for k in range(4):
        await_send(k)

    def drain(u, _):
        await_cross(u // PLANE, u % PLANE)
        return 0

    lax.fori_loop(0, 2 * PLANE, drain, 0)
    lax.fori_loop(4 * PLANE - WINDOW, 4 * PLANE, drain, 0)
    swap.wait_send()
    take(gpeer.at[pl.ds(0, PLANE - 1)], send_sem.at[5])
    take(gz.at[pl.ds(0, 7)], send_sem.at[6])
    take(gzag.at[pl.ds(0, 7)], send_sem.at[7])
    take(grads_ref.at[0, pl.ds(0, PLANE - 1)], send_sem.at[8])
    give.wait_send()


def copy_out(*refs):
    n = len(refs) // 2
    copies = [pltpu.make_async_copy(refs[i], refs[n + i], refs[-1].at[i]) for i in range(n)]
    for c in copies:
        c.start()
    for c in copies:
        c.wait()


def shards(tokens, cotangent, in_weight, in_bias, out_weight, out_bias):
    const = [jnp.asarray(a, BF) for a in constants()]
    vm = pl.BlockSpec(memory_space=pltpu.VMEM)
    hb = pl.BlockSpec(memory_space=pl.ANY)
    V = pltpu.VMEM
    local = (3, COLS, 2, D)
    results = pl.pallas_call(
        kernel,
        out_shape=(
            V(local, BF), V(local, BF),
            V(in_weight.shape, F32), V(in_bias.shape, F32),
            V(out_weight.shape, F32), V(out_bias.shape, F32),
        ),
        in_specs=[hb, hb, vm, hb, hb, hb, hb, hb, vm, vm],
        out_specs=(vm,) * 6,
        scratch_shapes=[
            V(local, BF), V(local, BF), V((3 * PADR, D), BF), V((3 * PADR, D), BF),
            V((2, PLANE, 4, 8, HALF), BF),
            V((PADR, 128), BF), V((2 * ROWS, ALL), BF), V((ALL, 256), BF), V((2, 2, 8, 96, 96), BF),
            V((ALL, 3 * PADR), BF), V((3 * PADR, ALL), BF),
            V((ALL, ALL), BF), V((ALL, ALL), BF),
            V((2, 2, 2, HALF, HALF), BF),
            V((4, SLOTS, PIECE, D), BF), V((4, SLOTS, PIECE, D), BF),
            V((ALL, D), BF), V((ALL, D), F32), V((ALL, D), BF),
            V((2, ALL, ALL), BF), V((2, ALL, ALL), BF), V((ALL, D), BF),
            V((2, PLANE, 32, HALF), F32), V((PLANE, 32, HALF), F32),
            V((PLANE, 32, HALF), F32), V((4, 8, HALF), F32), V((8, 8, 256), F32),
            V((8, 256), F32), V((8, 8, 256), F32), V((4, 8, HALF), BF),
            pltpu.SemaphoreType.DMA((2, 3)), pltpu.SemaphoreType.DMA((5,)),
            pltpu.SemaphoreType.DMA((4, PLANE)),
            pltpu.SemaphoreType.DMA((10,)), pltpu.SemaphoreType.DMA((10,)),
        ],
        compiler_params=pltpu.CompilerParams(
            collective_id=0, has_side_effects=True, vmem_limit_bytes=54 * 1024 * 1024),
        name="afno",
    )(tokens.transpose(1, 2, 0, 3), cotangent.transpose(1, 2, 0, 3), *const,
      in_weight, out_weight, in_bias, out_bias)
    mixed, tgrad, *grads = pl.pallas_call(
        copy_out,
        out_shape=[jax.ShapeDtypeStruct(a.shape, a.dtype) for a in results],
        in_specs=[vm] * 6,
        out_specs=[hb] * 6,
        scratch_shapes=[pltpu.SemaphoreType.DMA((6,))],
        compiler_params=pltpu.CompilerParams(vmem_limit_bytes=1024 * 1024),
        name="copy_out",
    )(*[pltpu.with_memory_space_constraint(a, pltpu.VMEM) for a in results])
    mixed, tgrad = (a.transpose(2, 0, 1, 3) for a in (mixed, tgrad))
    return mixed, tgrad, *grads


def solution(mesh):
    in_specs = (P("rep", "seq", None, None), P("rep", "seq", None, None), P(), P(), P(), P())
    out_specs = (P("rep", "seq", None, None), P("rep", "seq", None, None), P(), P(), P(), P())
    return jax.shard_map(shards, mesh=mesh, in_specs=in_specs, out_specs=out_specs, check_vma=False)
```

```python
import functools
import math

import jax
import jax.numpy as jnp
import numpy as np
from jax import lax
from jax.experimental import pallas as pl
from jax.experimental.pallas import tpu as pltpu
from jax.sharding import PartitionSpec as P

BF = jnp.bfloat16
F32 = jnp.float32
MESH = pl.DeviceIdType.MESH

SLOTS = 32
PLANE = 16
PIECE = 24
ALL = SLOTS * PIECE
D = 768
HALF = 384
COLS = 180
PADR = 384
USED = 360
ROWS = 96
WINDOW = 6
NT = (((1,), (1,)), ((), ()))
TN = (((0,), (0,)), ((), ()))


def tables(length, modes):
    residue = np.arange(length)[:, None] * np.arange(modes)[None, :] % length
    angles = residue.astype(np.float32) * np.float32(2.0 * math.pi / length)
    factor = np.float32(1.0 / math.sqrt(length))
    return np.cos(angles) * factor, np.sin(angles) * factor


def constants():
    cos_c, sin_c = tables(COLS, 64)
    col = np.zeros((128, PADR), np.float32)
    col[0::2, :USED] = np.repeat(cos_c.T, 2, axis=1)
    col[1::2, :USED] = np.repeat(-sin_c.T, 2, axis=1)
    row = np.arange(ALL)
    slot, grid_row, part = row // 24, row // 2 % 3, row % 2
    cos_r, sin_r = tables(ROWS, ROWS)
    device = slot % 16 // 4 * 8 + slot // 16 * 4 + slot % 4
    h = device * 3 + grid_row
    rows_re = np.where(part[None] == 0, cos_r.T[:, h], sin_r.T[:, h])
    rows_im = np.where(part[None] == 0, -sin_r.T[:, h], cos_r.T[:, h])
    mixt = np.zeros((ALL, 256), np.float32)
    mixt[:, 0:ROWS] = rows_re.T
    mixt[:, 128:128 + ROWS] = rows_im.T
    return col, col.T, np.concatenate([rows_re, rows_im]), mixt


def floor_div(v, n):
    return jnp.floor((v.astype(F32) + 0.5) * (1.0 / n)).astype(jnp.int32)


def class_mod4(v, n):
    return floor_div(v, n) & 3


def iota(shape, dim):
    return lax.broadcasted_iota(jnp.int32, shape, dim)


def dot(a, b, dims=(((1,), (0,)), ((), ()))):
    return lax.dot_general(a, b, dims, preferred_element_type=F32)


def kernel(
    tok_hbm, cot_hbm, col_ref, colt_hbm, mix_hbm, mixt_hbm, win_hbm, wout_hbm, bin_ref, bout_ref,
    mixed_ref, tgrad_ref, gwin_ref, gbin_ref, gwout_ref, gbout_ref,
    tok, cot, tokp, cotp, grads_ref, colt_ref, mix_ref, mixt_ref, wraw, fwd, inv, mrow, mback, wbd,
    send, recv, spec, dgelu, hid, incpair, prepair, work,
    gsrc, gpeer, grs, gplane, gz, gfin, gzag, gout,
    in_sem, table_sem, cross_sem, send_sem, recv_sem,
):
    me = lax.axis_index("seq")
    rep = lax.axis_index("rep")
    X, Z, Y = me // 8, (me // 4) % 2, me % 4
    xy = X * 4 + Y
    slot = Z * 16 + xy
    zl, core = rep // 2, rep % 2

    def seq_of(z, p):
        return (p // 4) * 8 + z * 4 + p % 4

    def remote(src, dst, k, **where):
        return pltpu.make_async_remote_copy(
            src_ref=src, dst_ref=dst, send_sem=send_sem.at[k], recv_sem=recv_sem.at[k],
            device_id=where, device_id_type=MESH,
        )

    def take(ref, sem):
        pltpu.make_async_copy(ref, ref, sem).wait()

    loads = [
        [pltpu.make_async_copy(src.at[h], dst.at[h], in_sem.at[i, h]) for h in range(3)]
        for i, (src, dst) in enumerate(((tok_hbm, tok), (cot_hbm, cot)))
    ]
    late = [
        pltpu.make_async_copy(src, dst, table_sem.at[i])
        for i, (src, dst) in enumerate((
            (colt_hbm, colt_ref), (mix_hbm, mix_ref), (mixt_hbm, mixt_ref),
            (win_hbm, wraw.at[0]), (wout_hbm, wraw.at[1])))
    ]
    for c in loads[0] + loads[1] + late:
        c.start()
    for ref in (tokp, cotp):
        for h in range(3):
            ref[h * PADR + 352:(h + 1) * PADR, :] = jnp.zeros((32, D), BF)

    barrier = pltpu.get_barrier_semaphore()

    def greet(t, _):
        p = lax.rem(me + t, SLOTS)
        pl.semaphore_signal(barrier, inc=1, device_id={"seq": p}, device_id_type=MESH)
        return 0

    lax.fori_loop(1, SLOTS, greet, 0)
    pl.semaphore_signal(barrier, inc=1, device_id={"rep": zl * 2 + 1 - core}, device_id_type=MESH)
    z_here = Z * 4 + zl

    def along_z(t):
        z = lax.rem(z_here + t, 8)
        return z, z // 4, z % 4

    def z_peer(t):
        z, hi, lo = along_z(t)
        return {"seq": seq_of(hi, xy), "rep": lo * 2 + core}

    for t in (1, 2, 3, 5, 6, 7):
        pl.semaphore_signal(barrier, inc=1, device_id=z_peer(t), device_id_type=MESH)

    def message_parts(v):
        cls = class_mod4(v, 6)
        pair = floor_div(v, 2)
        grid_row = pair - 3 * floor_div(v, 6)
        table_row = floor_div(v, 24) * 4 + (cls & 1) * 2 + (v & 1)
        return cls, cls >> 1, grid_row, table_row

    r = iota((ALL, 1), 0)
    row_class, row_s, row_h, row_t = message_parts(r)
    pick = jnp.where(iota((ALL, 128), 1) == row_t, 1.0, 0.0).astype(BF)
    picked = dot(pick, col_ref[...])
    picked = jnp.where((iota((1, PADR), 1) & 1) == row_s, picked, 0.0)
    for h in range(3):
        fwd[:, h * PADR:(h + 1) * PADR] = jnp.where(row_h == h, picked, 0.0).astype(BF)

    def pad(copies, data, ref):
        for h in range(3):
            copies[h].wait()
            ref[h * PADR:h * PADR + USED, :] = data[h].reshape(USED, D)

    pad(loads[0], tok, tokp)
    pl.semaphore_wait(barrier, SLOTS - 1 + 1 + 6)

    def await_cross(k, t):
        pltpu.make_async_copy(send.at[k, 0], send.at[k, 0], cross_sem.at[k, t]).wait()

    def cross(k, lo, hi, paced=False):
        def step(t, _):
            if paced:
                before = k * PLANE + t - WINDOW
                await_cross(before // PLANE, before % PLANE)
            p = lax.rem(xy + t, PLANE)
            pltpu.make_async_remote_copy(
                src_ref=send.at[k, (1 - Z) * PLANE + p], dst_ref=recv.at[k, slot],
                send_sem=cross_sem.at[k, t], recv_sem=recv_sem.at[k],
                device_id={"seq": seq_of(1 - Z, p)}, device_id_type=MESH).start()
            return 0

        lax.fori_loop(lo, hi, step, 0)

    def near(k):
        def step(t, _):
            p = lax.rem(xy + t, PLANE)
            remote(send.at[k, Z * PLANE + p], recv.at[k, slot], k, seq=seq_of(Z, p)).start()
            return 0

        lax.fori_loop(1, PLANE, step, 0)

    def store_half(k, z, lhs, rhs, scale):
        left = lhs[pl.ds(pl.multiple_of(z * HALF, HALF), HALF), :]

        def tile(n, _):
            at = pl.ds(pl.multiple_of(n * 256, 256), 256)
            out = dot(left, rhs[:, at])
            if scale is not None:
                out = out * scale
            send[k, pl.ds(z * PLANE, PLANE), :, at] = out.astype(BF).reshape(PLANE, PIECE, 256)
            return 0

        lax.fori_loop(0, 3, tile, 0)

    def exchange(k, lhs, rhs, scale, first=PLANE, paced=False, both=True):
        store_half(k, 1 - Z, lhs, rhs, scale(1 - Z) if scale else None)
        cross(k, 0, first, paced)
        store_half(k, Z, lhs, rhs, scale(Z) if scale else None)
        if both:
            near(k)
        recv[k, slot] = send[k, slot]

    def await_recv(k):
        take(recv.at[k, pl.ds(0, SLOTS - 1)], recv_sem.at[k])

    def await_send(k):
        take(send.at[k, pl.ds(0, PLANE - 1)], send_sem.at[k])

    exchange(0, fwd, tokp, None)
    pad(loads[1], cot, cotp)
    rr = iota((HALF, 1), 0)

    def cot_scale(z):
        first = (floor_div(rr, 24) == 0) & (class_mod4(rr, 6) % 2 == 0) & (z == 0)
        return jnp.where(first, 1.0, 2.0)

    held = jnp.where(z_here % 4 == 0, 11, jnp.where(z_here % 4 == 3, 14, PLANE))
    exchange(1, fwd, cotp, cot_scale, held)

    for c in late:
        c.wait()
    c768 = iota((1, ALL), 1)
    col_class, col_s, col_h, col_t = message_parts(c768)
    pickt = jnp.where(iota((128, ALL), 0) == col_t, 1.0, 0.0).astype(BF)
    pickedt = dot(colt_ref[...], pickt)
    pickedt = jnp.where((iota((PADR, 1), 0) & 1) == col_s, pickedt, 0.0)
    for h in range(3):
        inv[h * PADR:(h + 1) * PADR, :] = jnp.where(col_h == h, pickedt, 0.0).astype(BF)
    for e in range(2):
        part = mix_ref[e * ROWS:(e + 1) * ROWS, :].astype(F32)
        for cls in range(4):
            at = (e * 4 + cls) * ROWS
            mrow[at:at + ROWS, :] = jnp.where(col_class == cls, part, 0.0).astype(BF)
    lane_block = floor_div(iota((1, HALF), 1), 96)
    part = mixt_ref[...].astype(F32)
    for e in range(2):
        wide = jnp.concatenate([part[:, e * 128:e * 128 + ROWS]] * 4, axis=1)
        mback[:, e * HALF:(e + 1) * HALF] = jnp.where(row_class == lane_block, wide, 0.0).astype(BF)
    for n in range(4):
        shift = jnp.where(iota((96, HALF), 1) == iota((96, HALF), 0) + 96 * n, 1.0, 0.0).astype(BF)
        for t in range(2):
            for ri in range(2):
                for g in range(2):
                    wbd[t, ri, g, n * 96:(n + 1) * 96, :] = dot(
                        wraw[t, ri, g * 4 + n], shift).astype(BF)

    def along_rows(k, store):
        def tile(n, _):
            at = pl.ds(pl.multiple_of(n * 256, 256), 256)
            store(at, dot(mrow[...], recv[k, :, :, at].reshape(ALL, 256)).astype(BF))
            return 0

        lax.fori_loop(0, 3, tile, 0)

    await_recv(0)

    def keep_spec(at, v):
        spec[:, at] = v

    along_rows(0, keep_spec)
    root = math.sqrt(2.0 / math.pi)
    for g in range(2):
        lanes = pl.ds(g * HALF, HALF)
        u = dot(spec[:, lanes], wbd[0, 0, g])
        v = dot(spec[:, lanes], wbd[0, 1, g])
        for e in range(2):
            mine = slice(e * HALF, (e + 1) * HALF)
            if e == 0:
                pre = u[:HALF] - v[HALF:] + bin_ref[0:1, lanes]
            else:
                pre = v[:HALF] + u[HALF:] + bin_ref[1:2, lanes]
            sq = pre * pre
            th = jnp.tanh(root * pre * (1.0 + 0.044715 * sq))
            hid[mine, lanes] = (0.5 * pre * (1.0 + th)).astype(BF)
            dgelu[mine, lanes] = 0.5 * (1.0 + th) + 0.5 * pre * (1.0 - th * th) * (
                root * (1.0 + 3.0 * 0.044715 * sq))
    for g in range(2):
        lanes = pl.ds(g * HALF, HALF)
        u = dot(hid[:, lanes], wbd[1, 0, g])
        v = dot(hid[:, lanes], wbd[1, 1, g])
        work[0:HALF, lanes] = (u[:HALF] - v[HALF:] + bout_ref[0:1, lanes]).astype(BF)
        work[HALF:ALL, lanes] = (v[:HALF] + u[HALF:] + bout_ref[1:2, lanes]).astype(BF)

    def mode_scale(z):
        first = (class_mod4(rr, 6) % 2 == 0) & (slot == 0)
        return jnp.where(first, 1.0, 2.0)

    exchange(2, mback, work, mode_scale, 0)

    cross(1, held, PLANE)

    await_recv(1)

    def keep_inc(at, v):
        work[:, at] = v

    cross(2, 0, WINDOW)
    along_rows(1, keep_inc)
    cross(2, WINDOW, 8, True)

    def pair_up(dst, g, top, bottom):
        dst[g, 0:HALF, 0:HALF] = top
        dst[g, HALF:ALL, 0:HALF] = bottom
        dst[g, 0:HALF, HALF:ALL] = bottom
        dst[g, HALF:ALL, HALF:ALL] = -top

    gsrc[...] = jnp.zeros_like(gsrc)

    def param_grads(t, g, left, pair, bias):
        prod = dot(left[:, g * HALF:(g + 1) * HALF], pair[g], TN)
        for ri in range(2):
            acc = jnp.zeros((96, HALF), F32)
            for n in range(4):
                acc = acc + jnp.where(
                    lane_block == n, prod[n * 96:(n + 1) * 96, ri * HALF:(ri + 1) * HALF], 0.0)
            gsrc[g, t * 8 + ri * 4:t * 8 + ri * 4 + 4, 0:24, :] = acc.reshape(4, 24, HALF)
            gsrc[g, t * 2 + ri, 24:32, :] = jnp.broadcast_to(bias[ri], (8, HALF))

    for g in range(2):
        lanes = pl.ds(g * HALF, HALF)
        inc = work[:, lanes]
        pair_up(incpair, g, inc[:HALF], inc[HALF:])
        u = dot(inc, wbd[1, 0, g], NT)
        v = dot(inc, wbd[1, 1, g], NT)
        top = ((u[:HALF] + v[HALF:]) * dgelu[0:HALF, lanes]).astype(BF)
        bottom = ((u[HALF:] - v[:HALF]) * dgelu[HALF:ALL, lanes]).astype(BF)
        pair_up(prepair, g, top, bottom)
        cross(2, 8 + 3 * g, 11 + 3 * g, True)
        incf = inc.astype(F32)
        param_grads(1, g, hid, incpair,
                    [jnp.sum(incf[:HALF], axis=0, keepdims=True),
                     jnp.sum(incf[HALF:], axis=0, keepdims=True)])
        param_grads(0, g, spec, prepair,
                    [jnp.sum(top.astype(F32), axis=0, keepdims=True),
                     jnp.sum(bottom.astype(F32), axis=0, keepdims=True)])
    swap = remote(gsrc.at[1 - core], gpeer, 4, rep=zl * 2 + 1 - core)
    swap.start()
    cross(2, 14, PLANE, True)
    for g in range(2):
        lanes = pl.ds(g * HALF, HALF)
        pre = prepair[g, :, 0:HALF]
        u = dot(pre, wbd[0, 0, g], NT)
        v = dot(pre, wbd[0, 1, g], NT)
        work[0:HALF, lanes] = (u[:HALF] + v[HALF:]).astype(BF)
        work[HALF:ALL, lanes] = (u[HALF:] - v[:HALF]).astype(BF)

    swap.wait_recv()
    grs_own = gsrc.at[core]
    gpeer[...] = gpeer[...] + grs_own[...]

    def reduce_plane(t, _):
        p = lax.rem(xy + t, PLANE)
        remote(gpeer.at[p], grs.at[xy], 5, seq=seq_of(Z, p)).start()
        return 0

    lax.fori_loop(1, PLANE, reduce_plane, 0)
    exchange(3, mback, work, None, WINDOW, True, False)

    grs[xy] = gpeer[xy]
    take(grs.at[pl.ds(0, PLANE - 1)], recv_sem.at[5])
    gplane[...] = jnp.sum(grs[...], axis=0).reshape(4, 8, HALF)

    def piece(hi, lo):
        return gplane.at[lo, :, pl.ds(pl.multiple_of(hi * 128, 128), 256)]

    for t in range(1, 8):
        z, hi, lo = along_z(t)
        remote(piece(hi, lo), gz.at[z_here], 6, **z_peer(t)).start()
    near(3)
    cross(3, WINDOW, 13, True)
    gz[z_here] = gplane[zl, :, pl.ds(pl.multiple_of(Z * 128, 128), 256)]
    take(gz.at[pl.ds(0, 7)], recv_sem.at[6])
    gfin[...] = jnp.sum(gz[...], axis=0) * (1.0 / 16.0)
    for t in range(1, 8):
        remote(gfin, gzag.at[z_here], 7, **z_peer(t)).start()
    cross(3, 13, PLANE, True)
    gzag[z_here] = gfin[...]
    take(gzag.at[pl.ds(0, 7)], recv_sem.at[7])
    for t in range(4):
        gout[t, :, 0:256] = gzag[t].astype(BF)
        gout[t, :, 256:HALF] = gzag[4 + t, :, 128:256].astype(BF)

    def gather_plane(t, _):
        p = lax.rem(xy + t, PLANE)
        remote(gout, grads_ref.at[core, xy], 8, seq=seq_of(Z, p)).start()
        return 0

    lax.fori_loop(1, PLANE, gather_plane, 0)
    grads_ref[core, xy] = gout[...]

    def finish(k, data, out_ref):
        def tile(n, _):
            at = pl.ds(pl.multiple_of(n * 256, 256), 256)
            got = recv[k, :, :, at].reshape(ALL, 256)
            for h in range(3):
                back = dot(inv[h * PADR:(h + 1) * PADR, :], got)
                total = data[h * PADR:h * PADR + USED, at].astype(F32) + back[:USED]
                out_ref[h, :, :, at] = total.astype(BF).reshape(COLS, 2, 256)
            return 0

        lax.fori_loop(0, 3, tile, 0)

    def place_grads(g):
        for q in range(4):
            weight, bias = ((gwin_ref, gbin_ref), (gwout_ref, gbout_ref))[q // 2]
            wide = grads_ref[g, 4 * q:4 * q + 4, 0:3].astype(F32).reshape(96, HALF)
            for n in range(4):
                weight[q % 2, g * 4 + n] = wide[:, n * 96:(n + 1) * 96]
            bias[q % 2:q % 2 + 1, pl.ds(pl.multiple_of(g * HALF, 128), HALF)] = (
                grads_ref[g, q, 3].astype(F32)[0:1])

    await_recv(2)
    finish(2, tokp, mixed_ref)

    take(grads_ref.at[core, pl.ds(0, PLANE - 1)], recv_sem.at[8])
    give = remote(grads_ref.at[core], grads_ref.at[core], 9, rep=zl * 2 + 1 - core)
    give.start()
    place_grads(core)
    await_recv(3)
    finish(3, cotp, tgrad_ref)
    take(grads_ref.at[1 - core], recv_sem.at[9])
    place_grads(1 - core)

    for k in range(4):
        await_send(k)

    def drain(u, _):
        await_cross(u // PLANE, u % PLANE)
        return 0

    lax.fori_loop(0, 2 * PLANE, drain, 0)
    lax.fori_loop(4 * PLANE - WINDOW, 4 * PLANE, drain, 0)
    swap.wait_send()
    take(gpeer.at[pl.ds(0, PLANE - 1)], send_sem.at[5])
    take(gz.at[pl.ds(0, 7)], send_sem.at[6])
    take(gzag.at[pl.ds(0, 7)], send_sem.at[7])
    take(grads_ref.at[0, pl.ds(0, PLANE - 1)], send_sem.at[8])
    give.wait_send()


def copy_out(*refs):
    n = len(refs) // 2
    copies = [pltpu.make_async_copy(refs[i], refs[n + i], refs[-1].at[i]) for i in range(n)]
    for c in copies:
        c.start()
    for c in copies:
        c.wait()


def shards(tokens, cotangent, in_weight, in_bias, out_weight, out_bias):
    const = [jnp.asarray(a, BF) for a in constants()]
    vm = pl.BlockSpec(memory_space=pltpu.VMEM)
    hb = pl.BlockSpec(memory_space=pl.ANY)
    V = pltpu.VMEM
    local = (3, COLS, 2, D)
    results = pl.pallas_call(
        kernel,
        out_shape=(
            V(local, BF), V(local, BF),
            V(in_weight.shape, F32), V(in_bias.shape, F32),
            V(out_weight.shape, F32), V(out_bias.shape, F32),
        ),
        in_specs=[hb, hb, vm, hb, hb, hb, hb, hb, vm, vm],
        out_specs=(vm,) * 6,
        scratch_shapes=[
            V(local, BF), V(local, BF), V((3 * PADR, D), BF), V((3 * PADR, D), BF),
            V((2, PLANE, 4, 8, HALF), BF),
            V((PADR, 128), BF), V((2 * ROWS, ALL), BF), V((ALL, 256), BF), V((2, 2, 8, 96, 96), BF),
            V((ALL, 3 * PADR), BF), V((3 * PADR, ALL), BF),
            V((ALL, ALL), BF), V((ALL, ALL), BF),
            V((2, 2, 2, HALF, HALF), BF),
            V((4, SLOTS, PIECE, D), BF), V((4, SLOTS, PIECE, D), BF),
            V((ALL, D), BF), V((ALL, D), F32), V((ALL, D), BF),
            V((2, ALL, ALL), BF), V((2, ALL, ALL), BF), V((ALL, D), BF),
            V((2, PLANE, 32, HALF), F32), V((PLANE, 32, HALF), F32),
            V((PLANE, 32, HALF), F32), V((4, 8, HALF), F32), V((8, 8, 256), F32),
            V((8, 256), F32), V((8, 8, 256), F32), V((4, 8, HALF), BF),
            pltpu.SemaphoreType.DMA((2, 3)), pltpu.SemaphoreType.DMA((5,)),
            pltpu.SemaphoreType.DMA((4, PLANE)),
            pltpu.SemaphoreType.DMA((10,)), pltpu.SemaphoreType.DMA((10,)),
        ],
        compiler_params=pltpu.CompilerParams(
            collective_id=0, has_side_effects=True, vmem_limit_bytes=54 * 1024 * 1024),
        name="afno",
    )(tokens.transpose(1, 2, 0, 3), cotangent.transpose(1, 2, 0, 3), *const,
      in_weight, out_weight, in_bias, out_bias)
    mixed, tgrad, *grads = pl.pallas_call(
        copy_out,
        out_shape=[jax.ShapeDtypeStruct(a.shape, a.dtype) for a in results],
        in_specs=[vm] * 6,
        out_specs=[hb] * 6,
        scratch_shapes=[pltpu.SemaphoreType.DMA((6,))],
        compiler_params=pltpu.CompilerParams(vmem_limit_bytes=1024 * 1024),
        name="copy_out",
    )(*[pltpu.with_memory_space_constraint(a, pltpu.VMEM) for a in results])
    mixed, tgrad = (a.transpose(2, 0, 1, 3) for a in (mixed, tgrad))
    return mixed, tgrad, *grads


def solution(mesh):
    in_specs = (P("rep", "seq", None, None), P("rep", "seq", None, None), P(), P(), P(), P())
    out_specs = (P("rep", "seq", None, None), P("rep", "seq", None, None), P(), P(), P(), P())
    return jax.shard_map(shards, mesh=mesh, in_specs=in_specs, out_specs=out_specs, check_vma=False)
```
